32 devices in a mesh: blk: 8 (over y, x, core), wide: 4 (over z).
Axes of the slice: x: 2, y: 2, z: 4, core: 2. Of those that a mesh axis runs over, the one named last changes fastest.
Arguments:
- points: bfloat16 [8192, 32], P(('blk', 'wide')), may hold values from -6 to 6
- inv_length: float32 [32], replicated, may hold values from 0.2 to 0.7
- noise_var: float32 [], replicated, may hold values from 0.1 to 1
- solution: float32 [8192, 128], P(('blk', 'wide')), may hold values from -6 to 6
- residual: float32 [8192, 128], P(('blk', 'wide')), may hold values from -6 to 6
- direction: float32 [8192, 128], P(('blk', 'wide')), may hold values from -6 to 6
Outputs:
- new_solution: float32 [8192, 128], P(('blk', 'wide'))
- new_residual: float32 [8192, 128], P(('blk', 'wide'))
- new_direction: float32 [8192, 128], P(('blk', 'wide'))
The draws below stay inside these ranges and needn't reach their ends.
All inputs are finite; a program needn't handle non-finite values.
Results may differ from the reference program's by a relative error of at most 0.01.
Values may be sent and summed in bfloat16 or wider, within the bound.
A program may use at most 64 MiB of HBM per device.

```python
import math
import jax
import jax.numpy as jnp
from jax import lax

PIECE = 256
FEATURES = 32
RHS = 128
POINTS = 8192


def levels(rng, extent, shards, low, largest):
    def one(position, shards_of):
        steps = jax.random.uniform(jax.random.fold_in(jax.random.fold_in(rng, 6), position), (shards_of,), jnp.float32, low / len(shards), largest / len(shards))
        return jnp.repeat(jnp.exp(steps), extent[position] // shards_of).reshape((-1,) + (1,) * (len(extent) - position - 1))

    gain = one(*shards[0])
    for cut in shards[1:]:
        gain = gain * one(*cut)
    return gain


def noise(own_key, extent, spread, limit, cuts=(), kind=jnp.bfloat16):
    gain = levels(own_key, extent, cuts, -0.22, 0.18) if cuts else 1.0
    result = jax.random.normal(own_key, extent, jnp.float32) * spread * gain
    return jnp.minimum(jnp.maximum(result, -limit), limit).astype(kind)


def setup_inputs(seed: int = 0) -> dict:
    seeds = jax.random.split(jax.random.key(seed), 7)
    return {
        "points": noise(seeds[0], (POINTS, FEATURES), 1.0, 6.0, ((0, 32),)),
        "inv_length": jnp.clip(jnp.exp(jax.random.uniform(seeds[1], (FEATURES,), jnp.float32, math.log(0.2), math.log(0.7))), 0.2, 0.7),
        "noise_var": jnp.clip(jnp.exp(jax.random.uniform(seeds[2], (), jnp.float32, math.log(0.1), math.log(1.0))), 0.1, 1.0),
        "solution": noise(seeds[3], (POINTS, RHS), 1.0, 6.0, ((0, 32),), jnp.float32),
        "residual": noise(seeds[4], (POINTS, RHS), 1.0, 6.0, ((0, 32),), jnp.float32),
        "direction": noise(seeds[5], (POINTS, RHS), 1.0, 6.0, ((0, 32),), jnp.float32),
    }


def kernel_tile(rows_x, rows_sq, cols_x, cols_sq):
    inner_prod = jnp.dot(rows_x, cols_x.T, precision=lax.Precision.HIGHEST)
    dist_sq = jnp.maximum(rows_sq[:, None] + cols_sq[None, :] - 2.0 * inner_prod, 0.0)
    radius = jnp.sqrt(5.0 * dist_sq)
    rounded = ((1.0 + radius + radius * radius / 3.0) * jnp.exp(-radius)).astype(jnp.bfloat16)
    return lax.optimization_barrier(rounded).astype(jnp.float32)

def reference(points, inv_length, noise_var, solution, residual, direction):
    scaled = (points.astype(jnp.float32) * inv_length).astype(jnp.bfloat16)
    low_dir = direction.astype(jnp.bfloat16)
    wide_x = lax.optimization_barrier(scaled).astype(jnp.float32)
    wide_p = lax.optimization_barrier(low_dir).astype(jnp.float32)
    point_sq = lax.optimization_barrier(jnp.sum(wide_x * wide_x, axis=1))

    def row_block(block_index):
        start = (block_index * PIECE).astype(jnp.int32)
        rows_x = lax.dynamic_slice_in_dim(wide_x, start, PIECE, 0)
        rows_sq = lax.dynamic_slice_in_dim(point_sq, start, PIECE, 0)
        kernel_rows = kernel_tile(rows_x, rows_sq, wide_x, point_sq)
        return jnp.dot(kernel_rows, wide_p, precision=lax.Precision.HIGHEST)
    blocks = lax.map(row_block, jnp.arange(POINTS // PIECE, dtype=jnp.int32))
    kernel_image = blocks.reshape(POINTS, RHS) + noise_var * direction
    old_norm = lax.optimization_barrier(jnp.sum(residual * residual, axis=0))
    curvature = lax.optimization_barrier(jnp.sum(direction * kernel_image, axis=0))
    step_length = old_norm / curvature
    new_solution = solution + step_length * direction
    new_residual = residual - step_length * kernel_image
    new_norm = lax.optimization_barrier(jnp.sum(new_residual * new_residual, axis=0))
    new_direction = new_residual + new_norm / old_norm * direction
    return (new_solution, new_residual, new_direction)
```

```python
import functools
import math

import jax
import jax.numpy as jnp
from jax import lax
from jax.experimental import pallas as pl
from jax.experimental.pallas import tpu as pltpu
from jax.sharding import PartitionSpec as P

LN2 = math.log(2.0)
SCALE = 5.0 / (LN2 * LN2)
MESH = pl.DeviceIdType.MESH
TAIL = 16


def rounded(x):
    return x.astype(jnp.bfloat16).astype(jnp.float32)


def three_parts(x):
    high = rounded(x)
    rest = x - high
    middle = rounded(rest)
    return high, middle, rounded(rest - middle)


def matern(scaled_dist):
    dist = jnp.maximum(scaled_dist, 1e-30)
    root = dist * lax.rsqrt(dist)
    poly = 1.0 + root * (LN2 + (LN2 * LN2 / 3.0) * root)
    return (poly * jnp.exp2(-root)).astype(jnp.bfloat16)


def kernel(nb, nw, points, inv_length, noise_var, residual, direction, image, coef,
           feat, feat_z, rows_x, kmat, low_dir, part, part_in, stat, stat_z, stat_b, stat_o,
           fs, fr, fzs, fzr, ps, pr, qs, qr, zs, zr, bs, br):
    b = lax.axis_index("blk")
    w = lax.axis_index("wide")
    chips = nb // 2
    chip, core = b // 2, b % 2
    piece, features = points.shape

    def same_core(q):
        return (lax.rem(chip + q, chips) * 2 + core, w)

    sibling = (chip * 2 + 1 - core, w)

    def along(q):
        return (b, lax.rem(w + q, nw))

    def plane(slot):
        return (lax.rem(chip + slot // 2, chips) * 2 + (core if slot % 2 == 0 else 1 - core), w)

    def back(slot):
        return (chips - slot // 2) % chips * 2 + slot % 2

    barrier = pltpu.get_barrier_semaphore()
    for slot in range(1, nb):
        pl.semaphore_signal(barrier, inc=1, device_id=plane(slot), device_id_type=MESH)
    for q in range(1, nw):
        pl.semaphore_signal(barrier, inc=1, device_id=along(q), device_id_type=MESH)

    def copy(src, dst, send, recv, to):
        return pltpu.make_async_remote_copy(
            src_ref=src, dst_ref=dst, send_sem=send, recv_sem=recv, device_id=to, device_id_type=MESH
        )

    scaled = rounded(points[...].astype(jnp.float32) * inv_length[...])
    wide = jnp.concatenate([scaled, jnp.zeros((piece, 128 - features), jnp.float32)], axis=1)
    x_t = wide.T[:features]
    s1, s2, s3 = three_parts(SCALE * jnp.sum(x_t * x_t, axis=0, keepdims=True))
    row = lax.broadcasted_iota(jnp.int32, (TAIL, piece), 0)
    tail = jnp.where((row >= 3) & (row <= 10), 1.0, 0.0)
    tail = jnp.where((row >= 6) & (row <= 7), 0.0, tail)
    for at, value in ((0, s1), (1, s2), (2, s3), (11, s1), (12, s2), (13, s3)):
        tail = jnp.where(row == at, value, tail)
    feat[0] = jnp.concatenate([x_t, tail], axis=0).astype(jnp.bfloat16)
    low_dir[0:piece] = direction[...].astype(jnp.bfloat16)
    pl.semaphore_wait(barrier, nb - 1 + nw - 1)

    sends = []

    def go(c):
        c.start()
        sends.append(c)
        return c

    def feat_copy(src_slot, dst_slot, to):
        return copy(feat.at[src_slot], feat.at[dst_slot], fs.at[dst_slot], fr.at[dst_slot], to)

    def dir_copy(src_slot, dst_slot, to):
        return copy(low_dir.at[pl.ds(src_slot * piece, piece)], low_dir.at[pl.ds(dst_slot * piece, piece)],
                    ps.at[dst_slot], pr.at[dst_slot], to)

    for q in range(1, nw):
        go(copy(feat.at[0], feat_z.at[nw - q], fzs.at[q], fzr.at[nw - q], along(q)))
    go(feat_copy(0, 1, sibling))
    for q in range(1, chips):
        go(feat_copy(0, 2 * (chips - q), same_core(q)))
    for q in range(1, chips):
        go(dir_copy(0, 2 * (chips - q), same_core(q)))
    go(dir_copy(0, 1, sibling))

    def feat_arrived(slot):
        feat_copy(slot, slot, sibling).wait_recv()

    def dir_arrived(slot):
        dir_copy(slot, slot, sibling).wait_recv()

    def as_rows(block):
        block = block.astype(jnp.float32)
        x = block[:features]
        h, m, l = three_parts(SCALE * x)
        lanes = jnp.concatenate(
            [-2.0 * h, -2.0 * m, -2.0 * l, block[features + 8 :],
             jnp.zeros((TAIL + 8, piece), jnp.float32)], axis=0)
        return lanes.T.astype(jnp.bfloat16)

    rows_x[0:piece] = as_rows(feat[0])
    for q in range(1, nw):
        copy(feat_z.at[q], feat_z.at[q], fzs.at[q], fzr.at[q], along(q)).wait_recv()
        rows_x[q * piece : (q + 1) * piece] = as_rows(feat_z[q])

    depth = rows_x.shape[1]

    def tiles(slot):
        block = feat[slot]
        cols = jnp.concatenate(
            [block[:features]] * 3 + [block[features:],
             jnp.zeros((depth - 3 * features - TAIL, piece), jnp.bfloat16)], axis=0)

        def body(i, carry):
            at = pl.ds(pl.multiple_of(i * piece, piece), piece)
            dist = jnp.dot(rows_x[at, :], cols, preferred_element_type=jnp.float32)
            kmat[at, slot * piece : (slot + 1) * piece] = matern(dist)
            return carry

        lax.fori_loop(0, nw, body, 0, unroll=nw <= 4)

    for slot in range(nb):
        if slot > 0:
            feat_arrived(slot)
        if slot % 2 == 0:
            if slot > 0:
                go(feat_copy(slot, slot + 1, sibling))
        tiles(slot)
        if slot % 2 == 1 and slot >= nb - 5 and slot >= 3:
            pass
    for q in range(1, chips):
        dir_arrived(2 * q)
        go(dir_copy(2 * q, 2 * q + 1, sibling))
    for q in range(chips):
        dir_arrived(2 * q + 1)

    def partial(q):
        return jnp.dot(kmat[q * piece : (q + 1) * piece, :], low_dir[...],
                       preferred_element_type=jnp.float32)

    for q in range(1, nw):
        part[q] = partial(q).astype(jnp.bfloat16)
        go(copy(part.at[q], part_in.at[nw - q], qs.at[q], qr.at[nw - q], along(q)))
    total = partial(0) + noise_var[...] * direction[...]
    for q in range(1, nw):
        copy(part.at[q], part_in.at[q], qs.at[q], qr.at[q], along(q)).wait_recv()
        total = total + part_in[q].astype(jnp.float32)
    image[...] = total

    def column_sum(x):
        return jnp.sum(x, axis=0, keepdims=True)

    res, direc = residual[...], direction[...]
    at = lax.broadcasted_iota(jnp.int32, (8, res.shape[1]), 0)
    sums = jnp.zeros(at.shape, jnp.float32)
    for k, value in enumerate((res * res, direc * total, res * total, total * total)):
        sums = jnp.where(at == k, column_sum(value), sums)
    stat[...] = sums
    for q in range(1, nw):
        go(copy(stat, stat_z.at[nw - q], zs.at[q], zr.at[nw - q], along(q)))
    for q in range(1, nw):
        copy(stat, stat_z.at[q], zs.at[q], zr.at[q], along(q)).wait_recv()
        sums = sums + stat_z[q]
    stat_o[...] = sums
    for slot in range(1, nb):
        go(copy(stat_o, stat_b.at[back(slot)], bs.at[slot], br.at[back(slot)], plane(slot)))
    for slot in range(1, nb):
        copy(stat_o, stat_b.at[slot], bs.at[slot], br.at[slot], plane(slot)).wait_recv()
        sums = sums + stat_b[slot]
    coef[...] = sums
    for c in sends:
        c.wait_send()


def on_device(nb, nw, points, inv_length, noise_var, solution, residual, direction):
    piece, features = points.shape
    rhs = direction.shape[1]
    vmem = pl.BlockSpec(memory_space=pltpu.VMEM)
    dma = pltpu.SemaphoreType.DMA
    depth = 3 * features + 2 * TAIL
    image, coef = pl.pallas_call(
        functools.partial(kernel, nb, nw),
        out_shape=(
            jax.ShapeDtypeStruct((piece, rhs), jnp.float32),
            jax.ShapeDtypeStruct((8, rhs), jnp.float32),
        ),
        in_specs=[vmem] * 5,
        out_specs=(vmem, vmem),
        scratch_shapes=[
            pltpu.VMEM((nb, features + TAIL, piece), jnp.bfloat16),
            pltpu.VMEM((nw, features + TAIL, piece), jnp.bfloat16),
            pltpu.VMEM((nw * piece, depth), jnp.bfloat16),
            pltpu.VMEM((nw * piece, nb * piece), jnp.bfloat16),
            pltpu.VMEM((nb * piece, rhs), jnp.bfloat16),
            pltpu.VMEM((nw, piece, rhs), jnp.bfloat16),
            pltpu.VMEM((nw, piece, rhs), jnp.bfloat16),
            pltpu.VMEM((8, rhs), jnp.float32),
            pltpu.VMEM((nw, 8, rhs), jnp.float32),
            pltpu.VMEM((nb, 8, rhs), jnp.float32),
            pltpu.VMEM((8, rhs), jnp.float32),
            dma((nb,)), dma((nb,)), dma((nw,)), dma((nw,)), dma((nb,)), dma((nb,)),
            dma((nw,)), dma((nw,)), dma((nw,)), dma((nw,)), dma((nb,)), dma((nb,)),
        ],
        compiler_params=pltpu.CompilerParams(
            collective_id=0, has_side_effects=True, vmem_limit_bytes=60 * 1024 * 1024
        ),
    )(points, inv_length.reshape(1, features), noise_var.reshape(1, 1), residual, direction)
    old_norm, curvature, cross_term, image_norm = coef[0], coef[1], coef[2], coef[3]
    step_length = old_norm / curvature
    new_residual = residual - step_length * image
    new_norm = old_norm - 2.0 * step_length * cross_term + step_length * step_length * image_norm
    new_solution = solution + step_length * direction
    new_direction = new_residual + new_norm / old_norm * direction
    return (new_solution, new_residual, new_direction)


def solution(mesh):
    spec = P(("blk", "wide"), None)
    return jax.shard_map(
        functools.partial(on_device, mesh.shape["blk"], mesh.shape["wide"]),
        mesh=mesh,
        in_specs=(spec, P(), P(), spec, spec, spec),
        out_specs=(spec, spec, spec),
        check_vma=False,
    )
```

```python
import functools
import math

import jax
import jax.numpy as jnp
from jax import lax
from jax.experimental import pallas as pl
from jax.experimental.pallas import tpu as pltpu
from jax.sharding import PartitionSpec as P

LN2 = math.log(2.0)
SCALE = 5.0 / (LN2 * LN2)
MESH = pl.DeviceIdType.MESH
TAIL = 16


def rounded(x):
    return x.astype(jnp.bfloat16).astype(jnp.float32)


def three_parts(x):
    high = rounded(x)
    rest = x - high
    middle = rounded(rest)
    return high, middle, rounded(rest - middle)


def matern(scaled_dist):
    dist = jnp.maximum(scaled_dist, 1e-30)
    root = dist * lax.rsqrt(dist)
    poly = 1.0 + root * (LN2 + (LN2 * LN2 / 3.0) * root)
    return (poly * jnp.exp2(-root)).astype(jnp.bfloat16)


def kernel(nb, nw, points_in, inv_in, noise_in, residual_in, direction_in, image_out, step_out, ratio_out,
           points, inv_length, noise_var, residual, direction, image, io, feat, feat_z, rows_x, kmat, low_dir, part, part_in, stat, stat_z, stat_b, stat_o,
           fs, fr, fzs, fzr, ps, pr, qs, qr, zs, zr, bs, br):
    b = lax.axis_index("blk")
    w = lax.axis_index("wide")
    chips = nb // 2
    chip, core = b // 2, b % 2
    features, piece = points.shape

    def same_core(q):
        return (lax.rem(chip + q, chips) * 2 + core, w)

    sibling = (chip * 2 + 1 - core, w)

    def along(q):
        return (b, lax.rem(w + q, nw))

    def plane(slot):
        return (lax.rem(chip + slot // 2, chips) * 2 + (core if slot % 2 == 0 else 1 - core), w)

    def back(slot):
        return (chips - slot // 2) % chips * 2 + slot % 2

    barrier = pltpu.get_barrier_semaphore()
    for slot in range(1, nb):
        pl.semaphore_signal(barrier, inc=1, device_id=plane(slot), device_id_type=MESH)
    for q in range(1, nw):
        pl.semaphore_signal(barrier, inc=1, device_id=along(q), device_id_type=MESH)

    def copy(src, dst, send, recv, to):
        return pltpu.make_async_remote_copy(
            src_ref=src, dst_ref=dst, send_sem=send, recv_sem=recv, device_id=to, device_id_type=MESH
        )

    loads = [
        pltpu.make_async_copy(src, dst, io.at[k])
        for k, (src, dst) in enumerate(
            ((points_in, points), (inv_in, inv_length), (direction_in, direction),
             (noise_in, noise_var), (residual_in, residual))
        )
    ]
    for load in loads:
        load.start()
    for load in loads[:2]:
        load.wait()

    inv_row = jnp.concatenate(
        [inv_length[...], jnp.zeros((1, 128 - features), jnp.float32)], axis=1)
    inv_column = jnp.broadcast_to(inv_row, (8, 128)).T[:features, 0:1]
    x_t = rounded(points[...].astype(jnp.float32) * inv_column)
    s1, s2, s3 = three_parts(SCALE * jnp.sum(x_t * x_t, axis=0, keepdims=True))
    row = lax.broadcasted_iota(jnp.int32, (TAIL, piece), 0)
    tail = jnp.where((row >= 3) & (row <= 10), 1.0, 0.0)
    tail = jnp.where((row >= 6) & (row <= 7), 0.0, tail)
    for at, value in ((0, s1), (1, s2), (2, s3), (11, s1), (12, s2), (13, s3)):
        tail = jnp.where(row == at, value, tail)
    feat[0] = jnp.concatenate([x_t, tail], axis=0).astype(jnp.bfloat16)
    for load in loads[2:]:
        load.wait()
    low_dir[0:piece] = direction[...].astype(jnp.bfloat16)
    pl.semaphore_wait(barrier, nb - 1 + nw - 1)

    sends = []

    def go(c):
        c.start()
        sends.append(c)
        return c

    def feat_copy(src_slot, dst_slot, to):
        return copy(feat.at[src_slot], feat.at[dst_slot], fs.at[dst_slot], fr.at[dst_slot], to)

    def dir_copy(src_slot, dst_slot, to):
        return copy(low_dir.at[pl.ds(src_slot * piece, piece)], low_dir.at[pl.ds(dst_slot * piece, piece)],
                    ps.at[dst_slot], pr.at[dst_slot], to)

    for q in range(1, nw):
        go(copy(feat.at[0], feat_z.at[nw - q], fzs.at[q], fzr.at[nw - q], along(q)))
    go(feat_copy(0, 1, sibling))
    for q in range(1, chips):
        go(feat_copy(0, 2 * (chips - q), same_core(q)))
    for q in range(1, chips):
        go(dir_copy(0, 2 * (chips - q), same_core(q)))
    go(dir_copy(0, 1, sibling))

    def feat_arrived(slot):
        feat_copy(slot, slot, sibling).wait_recv()

    def dir_arrived(slot):
        dir_copy(slot, slot, sibling).wait_recv()

    def as_rows(block):
        block = block.astype(jnp.float32)
        x = block[:features]
        h, m, l = three_parts(SCALE * x)
        lanes = jnp.concatenate(
            [-2.0 * h, -2.0 * m, -2.0 * l, block[features + 8 :],
             jnp.zeros((TAIL + 8, piece), jnp.float32)], axis=0)
        return lanes.T.astype(jnp.bfloat16)

    depth = rows_x.shape[1]

    def tile(at, slot):
        block = feat[slot]
        cols = jnp.concatenate(
            [block[:features]] * 3 + [block[features:],
             jnp.zeros((depth - 3 * features - TAIL, piece), jnp.bfloat16)], axis=0)
        dist = jnp.dot(rows_x[at, :], cols, preferred_element_type=jnp.float32)
        kmat[at, slot * piece : (slot + 1) * piece] = matern(dist)

    def feat_z_arrived(q):
        copy(feat_z.at[q], feat_z.at[q], fzs.at[q], fzr.at[q], along(q)).wait_recv()

    def relay_direction(q):
        dir_arrived(2 * q)
        go(dir_copy(2 * q, 2 * q + 1, sibling))

    rows_x[0:piece] = as_rows(feat[0])
    tile(pl.ds(0, piece), 0)
    feat_arrived(1)
    tile(pl.ds(0, piece), 1)
    for q in range(1, chips):
        feat_arrived(2 * q)
        go(feat_copy(2 * q, 2 * q + 1, sibling))
        tile(pl.ds(0, piece), 2 * q)
    for q in range(1, chips):
        feat_arrived(2 * q + 1)
        tile(pl.ds(0, piece), 2 * q + 1)
    if nw <= 4:
        relayed = 1
        for q in range(1, nw):
            feat_z_arrived(q)
            rows_x[q * piece : (q + 1) * piece] = as_rows(feat_z[q])
            for slot in range(nb):
                tile(pl.ds(q * piece, piece), slot)
                if q == nw - 1 and slot in (0, nb // 2) and relayed < chips:
                    relay_direction(relayed)
                    relayed += 1
    else:
        relayed = 1
        for q in range(1, nw):
            feat_z_arrived(q)
            rows_x[q * piece : (q + 1) * piece] = as_rows(feat_z[q])

        def row_tiles(q, carry):
            for slot in range(nb):
                tile(pl.ds(pl.multiple_of(q * piece, piece), piece), slot)
            return carry

        lax.fori_loop(1, nw, row_tiles, 0)
    for q in range(relayed, chips):
        relay_direction(q)
    for q in range(chips):
        dir_arrived(2 * q + 1)

    def partial(q):
        return jnp.dot(kmat[q * piece : (q + 1) * piece, :], low_dir[...],
                       preferred_element_type=jnp.float32)

    for q in range(1, nw):
        part[q] = partial(q).astype(jnp.bfloat16)
        go(copy(part.at[q], part_in.at[nw - q], qs.at[q], qr.at[nw - q], along(q)))
    total = partial(0) + noise_var[...] * direction[...]
    for q in range(1, nw):
        copy(part.at[q], part_in.at[q], qs.at[q], qr.at[q], along(q)).wait_recv()
        total = total + part_in[q].astype(jnp.float32)
    image[...] = total
    store = pltpu.make_async_copy(image, image_out, io.at[5])
    store.start()

    def column_sum(x):
        return jnp.sum(x, axis=0, keepdims=True)

    res, direc = residual[...], direction[...]
    at = lax.broadcasted_iota(jnp.int32, (8, res.shape[1]), 0)
    sums = jnp.zeros(at.shape, jnp.float32)
    for k, value in enumerate((res * res, direc * total, res * total, total * total)):
        sums = jnp.where(at == k, column_sum(value), sums)
    stat[...] = sums
    for q in range(1, nw):
        go(copy(stat, stat_z.at[nw - q], zs.at[q], zr.at[nw - q], along(q)))
    for q in range(1, nw):
        copy(stat, stat_z.at[q], zs.at[q], zr.at[q], along(q)).wait_recv()
        sums = sums + stat_z[q]
    stat_o[...] = sums
    for slot in range(1, nb):
        go(copy(stat_o, stat_b.at[back(slot)], bs.at[slot], br.at[back(slot)], plane(slot)))
    for slot in range(1, nb):
        copy(stat_o, stat_b.at[slot], bs.at[slot], br.at[slot], plane(slot)).wait_recv()
        sums = sums + stat_b[slot]
    old_norm, step = sums[0:1], sums[0:1] / sums[1:2]
    new_norm = old_norm - 2.0 * step * sums[2:3] + step * step * sums[3:4]
    step_out[...] = step
    ratio_out[...] = new_norm / old_norm
    store.wait()
    for c in sends:
        c.wait_send()


def on_device(nb, nw, points, inv_length, noise_var, solution, residual, direction):
    piece, features = points.shape
    rhs = direction.shape[1]
    vmem = pl.BlockSpec(memory_space=pltpu.VMEM)
    hbm = pl.BlockSpec(memory_space=pl.ANY)
    dma = pltpu.SemaphoreType.DMA
    depth = 3 * features + 2 * TAIL
    image, step_length, ratio = pl.pallas_call(
        functools.partial(kernel, nb, nw),
        out_shape=(
            jax.ShapeDtypeStruct((piece, rhs), jnp.float32),
            jax.ShapeDtypeStruct((1, rhs), jnp.float32),
            jax.ShapeDtypeStruct((1, rhs), jnp.float32),
        ),
        in_specs=[hbm] * 5,
        out_specs=(hbm, vmem, vmem),
        scratch_shapes=[
            pltpu.VMEM((features, piece), points.dtype),
            pltpu.VMEM((1, features), jnp.float32),
            pltpu.VMEM((1, 1), jnp.float32),
            pltpu.VMEM((piece, rhs), jnp.float32),
            pltpu.VMEM((piece, rhs), jnp.float32),
            pltpu.VMEM((piece, rhs), jnp.float32),
            dma((6,)),
            pltpu.VMEM((nb, features + TAIL, piece), jnp.bfloat16),
            pltpu.VMEM((nw, features + TAIL, piece), jnp.bfloat16),
            pltpu.VMEM((nw * piece, depth), jnp.bfloat16),
            pltpu.VMEM((nw * piece, nb * piece), jnp.bfloat16),
            pltpu.VMEM((nb * piece, rhs), jnp.bfloat16),
            pltpu.VMEM((nw, piece, rhs), jnp.bfloat16),
            pltpu.VMEM((nw, piece, rhs), jnp.bfloat16),
            pltpu.VMEM((8, rhs), jnp.float32),
            pltpu.VMEM((nw, 8, rhs), jnp.float32),
            pltpu.VMEM((nb, 8, rhs), jnp.float32),
            pltpu.VMEM((8, rhs), jnp.float32),
            dma((nb,)), dma((nb,)), dma((nw,)), dma((nw,)), dma((nb,)), dma((nb,)),
            dma((nw,)), dma((nw,)), dma((nw,)), dma((nw,)), dma((nb,)), dma((nb,)),
        ],
        compiler_params=pltpu.CompilerParams(
            collective_id=0, has_side_effects=True, vmem_limit_bytes=60 * 1024 * 1024
        ),
    )(points.T, inv_length.reshape(1, features), noise_var.reshape(1, 1), residual, direction)
    new_residual = residual - step_length * image
    new_solution = solution + step_length * direction
    new_direction = new_residual + ratio * direction
    return (new_solution, new_residual, new_direction)


def solution(mesh):
    spec = P(("blk", "wide"), None)
    return jax.shard_map(
        functools.partial(on_device, mesh.shape["blk"], mesh.shape["wide"]),
        mesh=mesh,
        in_specs=(spec, P(), P(), spec, spec, spec),
        out_specs=(spec, spec, spec),
        check_vma=False,
    )
```

```python
import functools
import math

import jax
import jax.numpy as jnp
from jax import lax
from jax.experimental import pallas as pl
from jax.experimental.pallas import tpu as pltpu
from jax.sharding import PartitionSpec as P

LN2 = math.log(2.0)
SCALE = 5.0 / (LN2 * LN2)
MESH = pl.DeviceIdType.MESH
TAIL = 16


def rounded(x):
    return x.astype(jnp.bfloat16).astype(jnp.float32)


def three_parts(x):
    high = rounded(x)
    rest = x - high
    middle = rounded(rest)
    return high, middle, rounded(rest - middle)


def matern(scaled_dist):
    dist = jnp.maximum(scaled_dist, 1e-30)
    root = dist * lax.rsqrt(dist)
    poly = 1.0 + root * (LN2 + (LN2 * LN2 / 3.0) * root)
    return (poly * jnp.exp2(-root)).astype(jnp.bfloat16)


def kernel(nb, nw, points_in, inv_in, noise_in, residual_in, direction_in, image_out, step_out, ratio_out,
           points, inv_length, noise_var, residual, direction, image, io, feat, feat_z, rows_x, kmat, low_dir, part, part_in, stat, stat_z, stat_b, stat_o,
           fs, fr, fzs, fzr, ps, pr, qs, qr, zs, zr, bs, br):
    b = lax.axis_index("blk")
    w = lax.axis_index("wide")
    chips = nb // 2
    chip, core = b // 2, b % 2
    features, piece = points.shape

    def same_core(q):
        return (lax.rem(chip + q, chips) * 2 + core, w)

    sibling = (chip * 2 + 1 - core, w)

    def along(q):
        return (b, lax.rem(w + q, nw))

    def plane(slot):
        return (lax.rem(chip + slot // 2, chips) * 2 + (core if slot % 2 == 0 else 1 - core), w)

    def back(slot):
        return (chips - slot // 2) % chips * 2 + slot % 2

    barrier = pltpu.get_barrier_semaphore()
    for slot in range(1, nb):
        pl.semaphore_signal(barrier, inc=1, device_id=plane(slot), device_id_type=MESH)
    for q in range(1, nw):
        pl.semaphore_signal(barrier, inc=1, device_id=along(q), device_id_type=MESH)

    def copy(src, dst, send, recv, to):
        return pltpu.make_async_remote_copy(
            src_ref=src, dst_ref=dst, send_sem=send, recv_sem=recv, device_id=to, device_id_type=MESH
        )

    loads = [
        pltpu.make_async_copy(src, dst, io.at[k])
        for k, (src, dst) in enumerate(
            ((points_in, points), (inv_in, inv_length), (direction_in, direction),
             (noise_in, noise_var), (residual_in, residual))
        )
    ]
    for load in loads:
        load.start()
    for load in loads[:2]:
        load.wait()

    inv_row = jnp.concatenate(
        [inv_length[...], jnp.zeros((1, 128 - features), jnp.float32)], axis=1)
    inv_column = jnp.broadcast_to(inv_row, (8, 128)).T[:features, 0:1]
    x_t = rounded(points[...].astype(jnp.float32) * inv_column)
    s1, s2, s3 = three_parts(SCALE * jnp.sum(x_t * x_t, axis=0, keepdims=True))
    row = lax.broadcasted_iota(jnp.int32, (TAIL, piece), 0)
    tail = jnp.where((row >= 3) & (row <= 10), 1.0, 0.0)
    tail = jnp.where((row >= 6) & (row <= 7), 0.0, tail)
    for at, value in ((0, s1), (1, s2), (2, s3), (11, s1), (12, s2), (13, s3)):
        tail = jnp.where(row == at, value, tail)
    feat[0] = jnp.concatenate([x_t, tail], axis=0).astype(jnp.bfloat16)
    for load in loads[2:]:
        load.wait()
    low_dir[0:piece] = direction[...].astype(jnp.bfloat16)
    pl.semaphore_wait(barrier, nb - 1 + nw - 1)

    upper = lax.div(2 * w, nw)

    def near(k):
        return k + upper * (nw - 2 * k)

    def rows_at(q):
        return pl.ds(pl.multiple_of(q * piece, piece), piece)

    sends = []

    def go(c):
        c.start()
        sends.append(c)
        return c

    def feat_copy(src_slot, dst_slot, to):
        return copy(feat.at[src_slot], feat.at[dst_slot], fs.at[dst_slot], fr.at[dst_slot], to)

    def dir_copy(src_slot, dst_slot, to):
        return copy(low_dir.at[pl.ds(src_slot * piece, piece)], low_dir.at[pl.ds(dst_slot * piece, piece)],
                    ps.at[dst_slot], pr.at[dst_slot], to)

    for k in range(1, nw):
        q = near(nw - k)
        go(copy(feat.at[0], feat_z.at[nw - q], fzs.at[q], fzr.at[nw - q], along(q)))
    go(feat_copy(0, 1, sibling))
    for q in range(1, chips):
        go(feat_copy(0, 2 * (chips - q), same_core(q)))
    for q in range(1, chips):
        go(dir_copy(0, 2 * (chips - q), same_core(q)))
    go(dir_copy(0, 1, sibling))

    def feat_arrived(slot):
        feat_copy(slot, slot, sibling).wait_recv()

    def dir_arrived(slot):
        dir_copy(slot, slot, sibling).wait_recv()

    def as_rows(block):
        block = block.astype(jnp.float32)
        x = block[:features]
        h, m, l = three_parts(SCALE * x)
        lanes = jnp.concatenate(
            [-2.0 * h, -2.0 * m, -2.0 * l, block[features + 8 :],
             jnp.zeros((TAIL + 8, piece), jnp.float32)], axis=0)
        return lanes.T.astype(jnp.bfloat16)

    depth = rows_x.shape[1]

    def tile(at, slot):
        block = feat[slot]
        cols = jnp.concatenate(
            [block[:features]] * 3 + [block[features:],
             jnp.zeros((depth - 3 * features - TAIL, piece), jnp.bfloat16)], axis=0)
        dist = jnp.dot(rows_x[at, :], cols, preferred_element_type=jnp.float32)
        kmat[at, slot * piece : (slot + 1) * piece] = matern(dist)

    def feat_z_arrived(q):
        copy(feat_z.at[q], feat_z.at[q], fzs.at[q], fzr.at[q], along(q)).wait_recv()

    def relay_direction(q):
        dir_arrived(2 * q)
        go(dir_copy(2 * q, 2 * q + 1, sibling))

    rows_x[0:piece] = as_rows(feat[0])
    tile(pl.ds(0, piece), 0)
    feat_arrived(1)
    tile(pl.ds(0, piece), 1)
    for q in range(1, chips):
        feat_arrived(2 * q)
        go(feat_copy(2 * q, 2 * q + 1, sibling))
        tile(pl.ds(0, piece), 2 * q)
    for q in range(1, chips):
        feat_arrived(2 * q + 1)
        tile(pl.ds(0, piece), 2 * q + 1)
    if nw <= 4:
        relayed = 1
        for k in range(1, nw):
            q = near(k)
            feat_z_arrived(q)
            rows_x[rows_at(q), :] = as_rows(feat_z[q])
            for slot in range(nb):
                tile(rows_at(q), slot)
                if k == nw - 1 and slot in (0, nb // 2) and relayed < chips:
                    relay_direction(relayed)
                    relayed += 1
    else:
        relayed = 1
        for q in range(1, nw):
            feat_z_arrived(q)
            rows_x[q * piece : (q + 1) * piece] = as_rows(feat_z[q])

        def row_tiles(q, carry):
            for slot in range(nb):
                tile(pl.ds(pl.multiple_of(q * piece, piece), piece), slot)
            return carry

        lax.fori_loop(1, nw, row_tiles, 0)
    for q in range(relayed, chips):
        relay_direction(q)
    for q in range(chips):
        dir_arrived(2 * q + 1)

    def partial(q):
        return jnp.dot(kmat[rows_at(q), :], low_dir[...],
                       preferred_element_type=jnp.float32)

    for k in range(1, nw):
        q = near(nw - k)
        part[q] = partial(q).astype(jnp.bfloat16)
        go(copy(part.at[q], part_in.at[nw - q], qs.at[q], qr.at[nw - q], along(q)))
    total = partial(0) + noise_var[...] * direction[...]
    for q in range(1, nw):
        copy(part.at[q], part_in.at[q], qs.at[q], qr.at[q], along(q)).wait_recv()
        total = total + part_in[q].astype(jnp.float32)
    image[...] = total
    store = pltpu.make_async_copy(image, image_out, io.at[5])
    store.start()

    def column_sum(x):
        return jnp.sum(x, axis=0, keepdims=True)

    res, direc = residual[...], direction[...]
    at = lax.broadcasted_iota(jnp.int32, (8, res.shape[1]), 0)
    sums = jnp.zeros(at.shape, jnp.float32)
    for k, value in enumerate((res * res, direc * total, res * total, total * total)):
        sums = jnp.where(at == k, column_sum(value), sums)
    stat[...] = sums
    for q in range(1, nw):
        go(copy(stat, stat_z.at[nw - q], zs.at[q], zr.at[nw - q], along(q)))
    for q in range(1, nw):
        copy(stat, stat_z.at[q], zs.at[q], zr.at[q], along(q)).wait_recv()
        sums = sums + stat_z[q]
    stat_o[...] = sums
    for slot in range(1, nb):
        go(copy(stat_o, stat_b.at[back(slot)], bs.at[slot], br.at[back(slot)], plane(slot)))
    for slot in range(1, nb):
        copy(stat_o, stat_b.at[slot], bs.at[slot], br.at[slot], plane(slot)).wait_recv()
        sums = sums + stat_b[slot]
    old_norm, step = sums[0:1], sums[0:1] / sums[1:2]
    new_norm = old_norm - 2.0 * step * sums[2:3] + step * step * sums[3:4]
    step_out[...] = step
    ratio_out[...] = new_norm / old_norm
    store.wait()
    for c in sends:
        c.wait_send()


def on_device(nb, nw, points, inv_length, noise_var, solution, residual, direction):
    piece, features = points.shape
    rhs = direction.shape[1]
    vmem = pl.BlockSpec(memory_space=pltpu.VMEM)
    hbm = pl.BlockSpec(memory_space=pl.ANY)
    dma = pltpu.SemaphoreType.DMA
    depth = 3 * features + 2 * TAIL
    image, step_length, ratio = pl.pallas_call(
        functools.partial(kernel, nb, nw),
        out_shape=(
            jax.ShapeDtypeStruct((piece, rhs), jnp.float32),
            jax.ShapeDtypeStruct((1, rhs), jnp.float32),
            jax.ShapeDtypeStruct((1, rhs), jnp.float32),
        ),
        in_specs=[hbm] * 5,
        out_specs=(hbm, vmem, vmem),
        scratch_shapes=[
            pltpu.VMEM((features, piece), points.dtype),
            pltpu.VMEM((1, features), jnp.float32),
            pltpu.VMEM((1, 1), jnp.float32),
            pltpu.VMEM((piece, rhs), jnp.float32),
            pltpu.VMEM((piece, rhs), jnp.float32),
            pltpu.VMEM((piece, rhs), jnp.float32),
            dma((6,)),
            pltpu.VMEM((nb, features + TAIL, piece), jnp.bfloat16),
            pltpu.VMEM((nw, features + TAIL, piece), jnp.bfloat16),
            pltpu.VMEM((nw * piece, depth), jnp.bfloat16),
            pltpu.VMEM((nw * piece, nb * piece), jnp.bfloat16),
            pltpu.VMEM((nb * piece, rhs), jnp.bfloat16),
            pltpu.VMEM((nw, piece, rhs), jnp.bfloat16),
            pltpu.VMEM((nw, piece, rhs), jnp.bfloat16),
            pltpu.VMEM((8, rhs), jnp.float32),
            pltpu.VMEM((nw, 8, rhs), jnp.float32),
            pltpu.VMEM((nb, 8, rhs), jnp.float32),
            pltpu.VMEM((8, rhs), jnp.float32),
            dma((nb,)), dma((nb,)), dma((nw,)), dma((nw,)), dma((nb,)), dma((nb,)),
            dma((nw,)), dma((nw,)), dma((nw,)), dma((nw,)), dma((nb,)), dma((nb,)),
        ],
        compiler_params=pltpu.CompilerParams(
            collective_id=0, has_side_effects=True, vmem_limit_bytes=60 * 1024 * 1024
        ),
    )(points.T, inv_length.reshape(1, features), noise_var.reshape(1, 1), residual, direction)
    new_residual = residual - step_length * image
    new_solution = solution + step_length * direction
    new_direction = new_residual + ratio * direction
    return (new_solution, new_residual, new_direction)


def solution(mesh):
    spec = P(("blk", "wide"), None)
    return jax.shard_map(
        functools.partial(on_device, mesh.shape["blk"], mesh.shape["wide"]),
        mesh=mesh,
        in_specs=(spec, P(), P(), spec, spec, spec),
        out_specs=(spec, spec, spec),
        check_vma=False,
    )
```
